32 devices in a mesh: dp: 4 (over y, core), vocab: 8 (over z, x).
Axes of the slice: x: 2, y: 2, z: 4, core: 2. Of those that a mesh axis runs over, the one named last changes fastest.
Arguments:
- student_hidden: bfloat16 [512, 2048], P('dp', 'vocab'), may hold values from -210 to 210
- student_blocks: bfloat16 [8, 1024, 4864], P('vocab', 'dp'), may hold values from -0.375 to 0.375
- teacher_logits: bfloat16 [512, 19456], P('dp', 'vocab'), may hold values from -16 to 308
- token_ids: int32 [512], P('dp'), may hold values from 0 to 19455
- loss_mask: int32 [512], P('dp'), may hold values from 0 to 1, as said below
Outputs:
- hidden_grad: bfloat16 [512, 2048], P('dp', 'vocab')
- token_kl: float32 [512], P('dp')
- sampled_logprob: float32 [512], P('dp')
- loss: float32 [], replicated
The draws below stay inside these ranges and needn't reach their ends.
Inputs may be any that keep to these rules, and one draw needn't show every extreme that they name: `loss_mask`: in each block of 128 tokens the mask is 0 on a leading run of at most 64 tokens and 1 on the rest.
All inputs are finite; a program needn't handle non-finite values.
Results may differ from the reference program's by a relative error of at most 0.0047.
Values may be sent and summed in bfloat16 or wider, within the bound.
No kernel may reach another device: no remote copies, remote signals or barrier semaphores. Data moves between devices by JAX's collectives and lax.ppermute only.
A program may use at most 64 MiB of HBM per device.

```python
import jax
import jax.numpy as jnp
from jax import lax

D = 2048
VT = 2432
TOK_DEV = 128
TOKENS = 512
V = 19456
N_VOCAB = 8


def draw_student_hidden(key, part):
    first_key = jax.random.fold_in(key, 0)
    values = jnp.clip(jax.random.normal(first_key, (TOKENS, D), jnp.float32), -6.0, 6.0)
    return values.astype(jnp.bfloat16)


def draw_teacher_logits(key, part):
    first_key = jax.random.fold_in(key, 0)
    return jnp.clip(3.0 * jax.random.normal(first_key, (TOKENS, V), jnp.float32), -16.0, 16.0).astype(jnp.bfloat16)


def draw_loss_mask(key, part):
    blocks = TOKENS // TOK_DEV
    starts = jax.random.randint(key, (blocks, 1), 0, TOK_DEV // 2 + 1)
    position = jnp.arange(TOK_DEV, dtype=jnp.int32)[None, :]
    return (position >= starts).astype(jnp.int32).reshape(TOKENS)


def set_ends(result, key, least, top_value):
    longest = result.shape.index(max(result.shape))
    spots = []
    for shift in (0, 1):
        where = [jax.random.randint(jax.random.fold_in(key, axis), (), 0, length) for axis, length in enumerate(result.shape)]
        where[longest] = (where[longest] + shift) % result.shape[longest]
        spots.append(tuple(where))
    return result.at[spots[0]].set(least).at[spots[1]].set(top_value)


def levels(stream_key, shape, cuts, least, high):
    gain = 1.0
    for dim, blocks in cuts:
        steps = jax.random.uniform(jax.random.fold_in(jax.random.fold_in(stream_key, 6), dim), (blocks,), jnp.float32, least / len(cuts), high / len(cuts))
        gain = gain * jnp.repeat(jnp.exp(steps), shape[dim] // blocks).reshape((-1,) + (1,) * (len(shape) - 1 - dim))
    return gain


def noise(stream_key, shape, scale, most, cuts=(), kind=jnp.bfloat16):
    array = scale * jax.random.normal(stream_key, shape, jnp.float32)
    if cuts:
        array = array * levels(stream_key, shape, cuts, -0.22, 0.18)
    return jnp.clip(array, -most, most).astype(kind)


def setup_inputs(seed: int = 0) -> dict:
    key_of = jax.random.split(jax.random.key(seed), 6)
    return {
        "student_hidden": draw_student_hidden(jax.random.fold_in(key_of[5], 71), 0),
        "student_blocks": noise(key_of[1], (N_VOCAB, D // 2, 2 * VT), (D // 9) ** -0.5, 0.375, ((0, 8), (1, 4))),
        "teacher_logits": draw_teacher_logits(jax.random.fold_in(key_of[5], 71), 0),
        "token_ids": set_ends(jax.random.randint(key_of[3], (TOKENS,), 0, V), jax.random.fold_in(key_of[3], 1), 0, V - 1).astype(jnp.int32),
        "loss_mask": draw_loss_mask(jax.random.fold_in(key_of[5], 71), 0),
    }


def reference(student_hidden, student_blocks, teacher_logits, token_ids, loss_mask):
    shards = N_VOCAB // 2
    width = 2 * VT
    weight = student_blocks.reshape(shards, 2, D // 2, width).transpose(1, 2, 0, 3).reshape(D, shards * width)
    mask_total = jnp.sum(loss_mask.astype(jnp.float32))

    def block(inputs):
        hidden, teacher, ids, mask = inputs
        logits = jnp.dot(hidden, weight, preferred_element_type=jnp.float32)
        student_logp = jax.nn.log_softmax(logits, axis=-1)
        teacher_logp = jax.nn.log_softmax(teacher.astype(jnp.float32), axis=-1)
        teacher_prob = jnp.exp(teacher_logp)
        kl_rows = jnp.sum(teacher_prob * (teacher_logp - student_logp), axis=-1)
        sampled = jnp.take_along_axis(student_logp, ids.astype(jnp.int32)[:, None], axis=1)[:, 0]
        factor = mask.astype(jnp.float32) / mask_total
        dlogits = (factor[:, None] * (jnp.exp(student_logp) - teacher_prob)).astype(jnp.bfloat16)
        grads = lax.dot_general(dlogits, weight, (((1,), (1,)), ((), ())), preferred_element_type=jnp.float32)
        return grads.astype(jnp.bfloat16), kl_rows, sampled

    blocks = TOKENS // TOK_DEV
    grads, kl_rows, sampled = lax.map(block, (student_hidden.reshape(blocks, TOK_DEV, D), teacher_logits.reshape(blocks, TOK_DEV, V), token_ids.reshape(blocks, TOK_DEV), loss_mask.reshape(blocks, TOK_DEV)))
    token_kl = kl_rows.reshape(TOKENS)
    loss = jnp.sum(loss_mask.astype(jnp.float32) * token_kl) / mask_total
    return grads.reshape(TOKENS, D), token_kl, sampled.reshape(TOKENS), loss
```

```python
import math

import jax
import jax.numpy as jnp
from jax import lax
from jax.sharding import Mesh, PartitionSpec as P

LANES = 128


def exchanged(array, **flips):
    axes = tuple(flips)
    sizes = [lax.axis_size(axis) for axis in axes]
    pairs = []
    for source in range(math.prod(sizes)):
        rest, target, stride = source, 0, 1
        for axis, size in reversed(list(zip(axes, sizes))):
            target += (rest % size ^ flips[axis]) * stride
            rest, stride = rest // size, stride * size
        pairs.append((source, target))
    return lax.ppermute(array, axes, pairs)


def cube_sum(value, axes):
    for axis in axes:
        for bit in range(lax.axis_size(axis).bit_length() - 1):
            value = value + exchanged(value, **{axis: 1 << bit})
    return value


def on_device(student_hidden, student_blocks, teacher_logits, token_ids, loss_mask):
    row_g, core, slab, half = (lax.axis_index(axis) for axis in ("g", "c", "s", "h"))
    n_g, n_s = lax.axis_size("g"), lax.axis_size("s")
    n_blocks = 4 * n_g
    tokens, feature = student_hidden.shape
    piece = student_blocks[0]
    rows = piece.shape[0]
    vt = piece.shape[1] // 2
    tiles = vt // LANES
    wide_tiles = -(-tiles // n_g)
    width = wide_tiles * LANES

    def offset(g):
        return (g * (tiles - wide_tiles)) // max(n_g - 1, 1) * LANES

    plane = [(mg, mh) for mg in range(n_g) for mh in range(2)]
    far_first = sorted(plane[1:], key=lambda m: (-(m[0] != 0) - m[1], m))

    hidden_plane = {(0, 0): student_hidden}
    for mg, mh in far_first:
        hidden_plane[mg, mh] = exchanged(student_hidden, g=mg, h=mh)

    def columns_of(g, h):
        start = pl_multiple(h * vt + offset(g))
        return lax.dynamic_slice_in_dim(piece, start, width, 1)

    blocks = {(0, 0, 0): columns_of(row_g, half)}
    for mg, mh in far_first:
        blocks[mg, mh, 0] = exchanged(columns_of(row_g ^ mg, half ^ mh), g=mg, h=mh)
    for mg, mh in [(0, 0)] + far_first:
        blocks[mg, mh, 1] = exchanged(blocks[mg, mh, 0], c=1)

    small = jnp.stack([token_ids, loss_mask])
    smalls = [small] + [exchanged(small, g=mg) for mg in range(1, n_g)]
    ids = jnp.concatenate([part[0] for part in smalls])
    mask_float = jnp.concatenate([part[1] for part in smalls]).astype(jnp.float32)
    core_total = jnp.full((8, LANES), jnp.sum(mask_float))
    mask_total = (core_total + exchanged(core_total, c=1))[0, 0]

    sides = [jnp.concatenate([hidden_plane[mg, mh] for mg in range(n_g)]) for mh in range(2)]
    plane_hidden = jnp.where(
        half == 0, jnp.concatenate(sides, axis=1), jnp.concatenate(sides[::-1], axis=1)
    )
    gathered = [plane_hidden] + [exchanged(plane_hidden, s=ms) for ms in range(1, n_s)]
    hidden = jnp.stack(gathered)

    def block_index(mg, mh, mc):
        return (half ^ mh) * 2 * n_g + 2 * (row_g ^ mg) + (core ^ mc)

    def hidden_of(index):
        pair = lax.dynamic_index_in_dim(hidden, slab ^ (index // 2), 0, False)
        return lax.dynamic_slice_in_dim(pair, index % 2 * feature, feature, 1)

    teacher = jnp.concatenate(
        [lax.dynamic_slice_in_dim(teacher_logits, offset(row_g), width, 1)]
        + [
            exchanged(lax.dynamic_slice_in_dim(teacher_logits, offset(row_g ^ mg), width, 1), g=mg)
            for mg in range(1, n_g)
        ]
    ).astype(jnp.float32)

    logits = None
    weight = jnp.zeros((n_blocks, rows, width), piece.dtype)
    for mg, mh in [(0, 0)] + far_first:
        for mc in range(2):
            block = blocks[mg, mh, mc]
            index = block_index(mg, mh, mc)
            if logits is not None:
                block, logits = lax.optimization_barrier((block, logits))
            term = jnp.dot(hidden_of(index), block, preferred_element_type=jnp.float32)
            logits = term if logits is None else logits + term
            place = index % 2 * n_s + index // 2
            weight = lax.dynamic_update_index_in_dim(weight, block, place, 0)

    local_column = lax.broadcasted_iota(jnp.int32, (1, width), 1)
    shared = jnp.where(row_g > 0, offset(row_g - 1) + width - offset(row_g), 0)
    mine = local_column >= shared
    low = jnp.float32(-3e38)
    student_max = jnp.max(jnp.where(mine, logits, low), axis=1)
    teacher_max = jnp.max(jnp.where(mine, teacher, low), axis=1)
    student_shift = logits - student_max[:, None]
    teacher_shift = teacher - teacher_max[:, None]
    student_sum = jnp.sum(jnp.where(mine, jnp.exp(student_shift), 0.0), axis=1)
    teacher_exp = jnp.where(mine, jnp.exp(teacher_shift), 0.0)
    teacher_sum = jnp.sum(teacher_exp, axis=1)
    cross = jnp.sum(teacher_exp * jnp.where(mine, teacher_shift - student_shift, 0.0), axis=1)
    column = local_column + (slab * 2 + half) * vt + offset(row_g)
    hit = (column == ids[:, None]) & mine
    picked = jnp.sum(jnp.where(hit, logits, 0.0), axis=1)

    stats = jnp.stack([student_max, student_sum, teacher_max, teacher_sum, cross, picked])
    stats = stats.reshape(6, n_g, tokens)

    def group(g):
        return lax.dynamic_index_in_dim(stats, g, 1, False)

    in_order = jnp.stack([group(row_g ^ g) for g in range(n_g)], 1)
    sent = jnp.broadcast_to(in_order, (n_g * n_s * 2,) + in_order.shape)
    every = lax.all_to_all(sent, ("g", "s", "h"), 0, 0, tiled=True)
    every = jnp.stack(
        [lax.dynamic_index_in_dim(every, row_g ^ mg, 2, False) for mg in range(n_g)], 2
    ).reshape(-1, 6, n_g * tokens)
    maxes, sums, t_maxes, t_sums, crosses, picks = (every[:, k] for k in range(6))
    top = jnp.max(maxes, axis=0)
    total = jnp.log(jnp.sum(sums * jnp.exp(maxes - top), axis=0))
    t_top = jnp.max(t_maxes, axis=0)
    t_scale = jnp.exp(t_maxes - t_top)
    t_total = jnp.sum(t_sums * t_scale, axis=0)
    t_log = jnp.log(t_total)

    student_logp = logits - top[:, None] - total[:, None]
    teacher_logp = teacher - t_top[:, None] - t_log[:, None]
    factor = (mask_float / mask_total)[:, None]
    delta = factor * (jnp.exp(student_logp) - jnp.exp(teacher_logp))
    dlogits = jnp.where(mine, delta, 0.0).astype(jnp.bfloat16)
    grads = lax.dot_general(
        dlogits,
        weight.reshape(n_blocks * rows, width),
        (((1,), (1,)), ((), ())),
        preferred_element_type=jnp.float32,
    )

    own = slice(0, tokens)
    gap = (t_maxes - t_top - t_log) - (maxes - top - total)
    token_kl = jnp.sum((t_scale * (crosses + t_sums * gap))[:, own], axis=0) / t_total[own]
    sampled = jnp.sum(picks[:, own], axis=0) - top[own] - total[own]
    loss_part = jnp.full((8, LANES), jnp.sum(mask_float[own] * token_kl))
    loss = cube_sum(loss_part, ("g", "c"))[0, 0] / mask_total

    def for_half(mg, h):
        group_rows = grads[mg * tokens : (mg + 1) * tokens]
        return lax.dynamic_slice_in_dim(group_rows, h * n_s * feature, n_s * feature, 1)

    partial = for_half(0, half)
    arrived = [
        exchanged(for_half(mg, half ^ mh).astype(jnp.bfloat16), g=mg, h=mh) for mg, mh in far_first
    ]
    for part in arrived:
        partial = partial + part.astype(jnp.float32)

    def for_slab(s):
        return lax.dynamic_slice_in_dim(partial, s * feature, feature, 1)

    result = for_slab(slab)
    arrived = [
        exchanged(for_slab(slab ^ ms).astype(jnp.bfloat16), s=ms) for ms in range(1, n_s)
    ]
    for part in arrived:
        result = result + part.astype(jnp.float32)
    return (result.astype(jnp.bfloat16), token_kl, sampled, loss)


def pl_multiple(start):
    return start // LANES * LANES


def solution(mesh):
    n_dp, n_vocab = mesh.devices.shape
    split = Mesh(mesh.devices.reshape(n_dp // 2, 2, n_vocab // 2, 2), ("g", "c", "s", "h"))
    dp, vocab = ("g", "c"), ("s", "h")
    return jax.shard_map(
        on_device,
        mesh=split,
        in_specs=(P(dp, vocab), P(vocab, dp, None), P(dp, vocab), P(dp), P(dp)),
        out_specs=(P(dp, vocab), P(dp), P(dp), P()),
        check_vma=False,
    )
```

```python
import math

import jax
import jax.numpy as jnp
from jax import lax
from jax.sharding import Mesh, PartitionSpec as P

LANES = 128


def exchanged(array, **flips):
    axes = tuple(flips)
    sizes = [lax.axis_size(axis) for axis in axes]
    pairs = []
    for source in range(math.prod(sizes)):
        rest, target, stride = source, 0, 1
        for axis, size in reversed(list(zip(axes, sizes))):
            target += (rest % size ^ flips[axis]) * stride
            rest, stride = rest // size, stride * size
        pairs.append((source, target))
    return lax.ppermute(array, axes, pairs)


def from_every(array, axes):
    return lax.all_to_all(array, axes, 0, 0, tiled=True)


def on_device(student_hidden, student_blocks, teacher_logits, token_ids, loss_mask):
    row_g, core, slab, half = (lax.axis_index(axis) for axis in ("g", "c", "s", "h"))
    n_g, n_s = lax.axis_size("g"), lax.axis_size("s")
    tokens, feature = student_hidden.shape
    piece = student_blocks[0]
    rows = piece.shape[0]
    vt = piece.shape[1] // 2
    tiles = vt // LANES
    wide_tiles = -(-tiles // n_g)
    width = wide_tiles * LANES

    def offset(g):
        return (g * (tiles - wide_tiles)) // max(n_g - 1, 1) * LANES

    plane = [(mg, mh) for mh in range(2) for mg in range(n_g)]
    far_first = sorted(plane[1:], key=lambda m: (-(m[0] != 0) - m[1], m))

    hidden_plane = {(0, 0): student_hidden}
    for mg, mh in far_first:
        hidden_plane[mg, mh] = exchanged(student_hidden, g=mg, h=mh)

    def columns_of(g, h):
        return lax.dynamic_slice_in_dim(piece, h * vt + offset(g), width, 1)

    blocks = {(0, 0, 0): columns_of(row_g, half)}
    for mg, mh in far_first:
        cut = columns_of(row_g ^ mg, half ^ mh)
        blocks[mg, mh, 0] = exchanged(cut, g=mg, h=mh)
    for mg, mh in [(0, 0)] + far_first:
        blocks[mg, mh, 1] = exchanged(blocks[mg, mh, 0], c=1)

    small = jnp.stack([token_ids, loss_mask])
    smalls = [small] + [exchanged(small, g=mg) for mg in range(1, n_g)]
    ids = jnp.concatenate([part[0] for part in smalls])
    mask_float = jnp.concatenate([part[1] for part in smalls]).astype(jnp.float32)
    core_total = jnp.full((8, LANES), jnp.sum(mask_float))
    mask_total = (core_total + exchanged(core_total, c=1))[0, 0]
    factor = (mask_float / mask_total)[:, None]

    local = teacher_logits.astype(jnp.float32)
    local_max = jnp.max(local, axis=1)
    local_sum = jnp.sum(jnp.exp(local - local_max[:, None]), axis=1)
    sent = jnp.broadcast_to(jnp.stack([local_max, local_sum]), (2 * n_s, 2, tokens))
    pairs = from_every(sent, ("s", "h"))
    t_top = jnp.max(pairs[:, 0], axis=0)
    t_log = jnp.log(jnp.sum(pairs[:, 1] * jnp.exp(pairs[:, 0] - t_top), axis=0))
    norm = jnp.stack([t_top, t_log])
    norms = [norm] + [exchanged(norm, g=mg) for mg in range(1, n_g)]
    t_top, t_log = jnp.concatenate(norms, axis=1)

    def teacher_of(g):
        return lax.dynamic_slice_in_dim(teacher_logits, offset(g), width, 1)

    teacher = jnp.concatenate(
        [teacher_of(row_g)]
        + [exchanged(teacher_of(row_g ^ mg), g=mg) for mg in range(1, n_g)]
    ).astype(jnp.float32)

    sides = [jnp.concatenate([hidden_plane[mg, mh] for mg in range(n_g)]) for mh in range(2)]
    plane_hidden = jnp.where(
        half == 0, jnp.concatenate(sides, axis=1), jnp.concatenate(sides[::-1], axis=1)
    )
    gathered = [plane_hidden]
    gathered += [exchanged(plane_hidden, s=ms) for ms in range(1, n_s)]
    hidden = jnp.stack(gathered)

    def hidden_of(mg, mh, mc):
        index = (half ^ mh) * 2 * n_g + 2 * (row_g ^ mg) + (core ^ mc)
        pair = lax.dynamic_index_in_dim(hidden, slab ^ (index // 2), 0, False)
        return lax.dynamic_slice_in_dim(pair, index % 2 * feature, feature, 1)

    logits = None
    for mg, mh in [(0, 0)] + far_first:
        for mc in range(2):
            block = blocks[mg, mh, mc]
            if logits is not None:
                block, logits = lax.optimization_barrier((block, logits))
            term = jnp.dot(hidden_of(mg, mh, mc), block, preferred_element_type=jnp.float32)
            logits = term if logits is None else logits + term

    local_column = lax.broadcasted_iota(jnp.int32, (1, width), 1)
    shared = jnp.where(row_g > 0, offset(row_g - 1) + width - offset(row_g), 0)
    mine = local_column >= shared

    def by_group(stack):
        parts = stack.reshape(stack.shape[0], n_g, tokens)
        return jnp.stack(
            [lax.dynamic_index_in_dim(parts, row_g ^ g, 1, False) for g in range(n_g)]
        )

    local_max = jnp.max(jnp.where(mine, logits, jnp.float32(-3e38)), axis=1)
    local_sum = jnp.sum(jnp.where(mine, jnp.exp(logits - local_max[:, None]), 0.0), axis=1)
    sent = by_group(jnp.stack([local_max, local_sum]))
    every = from_every(jnp.broadcast_to(sent, (2 * n_s * n_g,) + sent.shape), ("g", "s", "h"))
    every = jnp.concatenate(
        [lax.dynamic_index_in_dim(every, row_g ^ mg, 1, False) for mg in range(n_g)], 2
    )
    top = jnp.max(every[:, 0], axis=0)
    log_total = jnp.log(jnp.sum(every[:, 1] * jnp.exp(every[:, 0] - top), axis=0))

    student_logp = logits - top[:, None] - log_total[:, None]
    teacher_logp = teacher - t_top[:, None] - t_log[:, None]
    teacher_prob = jnp.exp(teacher_logp)
    delta = factor * (jnp.exp(student_logp) - teacher_prob)
    dlogits = jnp.where(mine, delta, 0.0).astype(jnp.bfloat16)

    weight = jnp.concatenate([blocks[mg, mh, mc] for mc in range(2) for mg, mh in plane])
    grads = lax.dot_general(
        dlogits, weight, (((1,), (1,)), ((), ())), preferred_element_type=jnp.float32
    )
    wide = len(plane) * rows

    def for_half(mg, mh):
        group_rows = grads[mg * tokens : (mg + 1) * tokens]
        return lax.dynamic_slice_in_dim(group_rows, (core ^ half ^ mh) * wide, wide, 1)

    partial = for_half(0, 0)
    arrived = [
        (exchanged(for_half(mg, mh).astype(jnp.bfloat16), g=mg, h=mh), mg, mh)
        for mg, mh in far_first
    ]
    for part, kg, kh in arrived:
        order = [(mh ^ kh) * n_g + (mg ^ kg) for mg, mh in plane]
        part = jnp.concatenate([part[:, j * rows : (j + 1) * rows] for j in order], axis=1)
        partial = partial + part.astype(jnp.float32)

    kl_part = jnp.sum(jnp.where(mine, teacher_prob * (teacher_logp - student_logp), 0.0), axis=1)
    column = local_column + (slab * 2 + half) * vt + offset(row_g)
    hit = (column == ids[:, None]) & mine
    picked = jnp.sum(jnp.where(hit, logits, 0.0), axis=1)
    loss_part = jnp.broadcast_to(jnp.sum(mask_float * kl_part), kl_part.shape)
    sent = by_group(jnp.stack([kl_part, picked, loss_part]))
    sent = jnp.broadcast_to(sent[:, None], (n_g, 2 * n_s) + sent.shape[1:])
    every = from_every(sent.reshape(-1, 3, tokens), ("g", "s", "h"))
    token_kl, picked, core_loss = jnp.sum(every, axis=0)
    sampled = picked - top[:tokens] - log_total[:tokens]
    core_loss = jnp.broadcast_to(core_loss, (8, LANES))
    loss = (core_loss + exchanged(core_loss, c=1))[0, 0] / mask_total

    def for_slab(s):
        index = (half ^ (s // n_g)) * n_g + (row_g ^ (s % n_g))
        return lax.dynamic_slice_in_dim(partial, index * rows, rows, 1)

    result = for_slab(slab)
    arrived = [exchanged(for_slab(slab ^ ms).astype(jnp.bfloat16), s=ms) for ms in range(1, n_s)]
    for part in arrived:
        result = result + part.astype(jnp.float32)
    return (result.astype(jnp.bfloat16), token_kl, sampled, loss)


def solution(mesh):
    n_dp, n_vocab = mesh.devices.shape
    n_g, n_s = n_dp // 2, n_vocab // 2
    split = Mesh(mesh.devices.reshape(n_g, 2, n_s, 2), ("g", "c", "s", "h"))
    dp, vocab = ("g", "c"), ("s", "h")
    return jax.shard_map(
        on_device,
        mesh=split,
        in_specs=(P(dp, vocab), P(vocab, dp, None), P(dp, vocab), P(dp), P(dp)),
        out_specs=(P(dp, vocab), P(dp), P(dp), P()),
        check_vma=False,
    )
```

```python
import math

import jax
import jax.numpy as jnp
from jax import lax
from jax.sharding import Mesh, PartitionSpec as P

LANES = 128


def exchanged(array, **flips):
    axes = tuple(flips)
    sizes = [lax.axis_size(axis) for axis in axes]
    pairs = []
    for source in range(math.prod(sizes)):
        rest, target, stride = source, 0, 1
        for axis, size in reversed(list(zip(axes, sizes))):
            target += (rest % size ^ flips[axis]) * stride
            rest, stride = rest // size, stride * size
        pairs.append((source, target))
    return lax.ppermute(array, axes, pairs)


def from_every(array, axes):
    return lax.all_to_all(array, axes, 0, 0, tiled=True)


def on_device(student_hidden, student_blocks, teacher_logits, token_ids, loss_mask):
    row_g, core, slab, half = (lax.axis_index(axis) for axis in ("g", "c", "s", "h"))
    n_g, n_s = lax.axis_size("g"), lax.axis_size("s")
    tokens, feature = student_hidden.shape
    piece = student_blocks[0]
    rows = piece.shape[0]
    vt = piece.shape[1] // 2
    tiles = vt // LANES
    wide_tiles = -(-tiles // n_g)
    width = wide_tiles * LANES

    def offset(g):
        return (g * (tiles - wide_tiles)) // max(n_g - 1, 1) * LANES

    plane = [(mg, mh) for mh in range(2) for mg in range(n_g)]
    others = sorted(plane[1:], key=lambda m: (m[0].bit_count() + m[1], m))

    hidden_plane = {(0, 0): student_hidden}
    for mg, mh in others:
        hidden_plane[mg, mh] = exchanged(student_hidden, g=mg, h=mh)

    def columns_of(g, h):
        return lax.dynamic_slice_in_dim(piece, h * vt + offset(g), width, 1)

    blocks = {(0, 0, 0): columns_of(row_g, half)}
    for mg, mh in others:
        cut = columns_of(row_g ^ mg, half ^ mh)
        blocks[mg, mh, 0] = exchanged(cut, g=mg, h=mh)
    for mg, mh in [(0, 0)] + others:
        blocks[mg, mh, 1] = exchanged(blocks[mg, mh, 0], c=1)

    local = teacher_logits.astype(jnp.float32)
    local_max = jnp.max(local, axis=1)
    local_sum = jnp.sum(jnp.exp(local - local_max[:, None]), axis=1)
    own_mask = loss_mask.astype(jnp.float32)
    own_count = jnp.full((8, LANES), jnp.sum(own_mask))
    chip_count = own_count + exchanged(own_count, c=1)
    own_parts = jnp.stack(
        [local_max, local_sum, own_mask + 2.0 * chip_count[0, 0], token_ids.astype(jnp.float32)]
    )

    def teacher_of(g):
        return lax.dynamic_slice_in_dim(teacher_logits, offset(g), width, 1)

    teacher = [teacher_of(row_g)] + [
        exchanged(teacher_of(row_g ^ mg), g=mg) for mg in range(1, n_g)
    ]

    sides = [jnp.concatenate([hidden_plane[mg, mh] for mg in range(n_g)]) for mh in range(2)]
    plane_hidden = jnp.where(
        half == 0, jnp.concatenate(sides, axis=1), jnp.concatenate(sides[::-1], axis=1)
    )
    gathered = [plane_hidden]
    gathered += [exchanged(plane_hidden, s=ms) for ms in range(1, n_s)]

    def hidden_of(mg, mh, mc):
        index = (half ^ mh) * n_g + (row_g ^ mg)
        pair = lax.select_n(slab ^ index, *gathered)
        return jnp.where((core ^ mc) == 0, pair[:, :feature], pair[:, feature:])

    logits = None
    for mg, mh in [(0, 0)] + others:
        for mc in range(2):
            block = blocks[mg, mh, mc]
            if logits is not None:
                block, logits = lax.optimization_barrier((block, logits))
            term = jnp.dot(hidden_of(mg, mh, mc), block, preferred_element_type=jnp.float32)
            logits = term if logits is None else logits + term

    local_column = lax.broadcasted_iota(jnp.int32, (1, width), 1)
    shared = jnp.where(row_g > 0, offset(row_g - 1) + width - offset(row_g), 0)
    mine = local_column >= shared

    def by_group(stack):
        parts = stack.reshape(stack.shape[0], n_g, tokens)
        return jnp.stack(
            [lax.dynamic_index_in_dim(parts, row_g ^ g, 1, False) for g in range(n_g)]
        )

    local_max = jnp.max(jnp.where(mine, logits, jnp.float32(-3e38)), axis=1)
    local_sum = jnp.sum(jnp.where(mine, jnp.exp(logits - local_max[:, None]), 0.0), axis=1)
    sent = by_group(jnp.stack([local_max, local_sum])).reshape(2 * n_g, tokens)
    sent = jnp.concatenate([sent, own_parts])
    every = from_every(jnp.broadcast_to(sent, (2 * n_s * n_g,) + sent.shape), ("g", "s", "h"))
    teacher, _ = lax.optimization_barrier((teacher, every))
    teacher = jnp.concatenate(teacher).astype(jnp.float32)
    student_parts = every[:, : 2 * n_g].reshape(2 * n_s * n_g, n_g, 2, tokens)
    student_parts = jnp.concatenate(
        [lax.dynamic_index_in_dim(student_parts, row_g ^ mg, 1, False) for mg in range(n_g)], 2
    )
    teacher_parts = every[:, 2 * n_g :].reshape(n_g, 2 * n_s, 4, tokens)
    teacher_parts = jnp.concatenate(
        [lax.dynamic_index_in_dim(teacher_parts, row_g ^ mg, 0, False) for mg in range(n_g)], 2
    )

    def normalizer(maxes, sums):
        top = jnp.max(maxes, axis=0)
        return top, jnp.log(jnp.sum(sums * jnp.exp(maxes - top), axis=0))

    top, log_total = normalizer(student_parts[:, 0], student_parts[:, 1])
    t_top, t_log = normalizer(teacher_parts[:, 0], teacher_parts[:, 1])
    coded, ids = teacher_parts[0, 2], teacher_parts[0, 3].astype(jnp.int32)
    chip_counts = jnp.floor(coded * 0.5)
    mask_float = coded - 2.0 * chip_counts
    mask_total = jnp.sum(chip_counts.reshape(n_g, tokens)[:, 0])
    factor = (mask_float / mask_total)[:, None]

    def log_probs(logits, teacher):
        student_logp = logits - top[:, None] - log_total[:, None]
        return student_logp, teacher - t_top[:, None] - t_log[:, None]

    student_logp, teacher_logp = log_probs(logits, teacher)
    delta = factor * (jnp.exp(student_logp) - jnp.exp(teacher_logp))
    dlogits = jnp.where(mine, delta, 0.0).astype(jnp.bfloat16)

    def features_of(mc, mg, mh):
        block = blocks[mg, mh, mc]
        return lax.dot_general(
            dlogits, block, (((1,), (1,)), ((), ())), preferred_element_type=jnp.float32
        )

    grads = [[features_of(mc, mg, mh) for mg, mh in plane] for mc in range(2)]
    crossed = (core ^ half) == 1

    def for_half(mg, mh):
        picks = [jnp.where(crossed, b, a) for a, b in zip(grads[mh], grads[1 - mh])]
        return jnp.concatenate([p[mg * tokens : (mg + 1) * tokens] for p in picks], axis=1)

    partial = for_half(0, 0)
    terms = [for_half(mg, mh).astype(jnp.bfloat16) for mg, mh in others]
    arrived = [(exchanged(term, g=mg, h=mh), mg, mh) for term, (mg, mh) in zip(terms, others)]
    for part, kg, kh in arrived:
        order = [(mh ^ kh) * n_g + (mg ^ kg) for mg, mh in plane]
        part = jnp.concatenate([part[:, j * rows : (j + 1) * rows] for j in order], axis=1)
        partial = partial + part.astype(jnp.float32)

    _, logits, teacher = lax.optimization_barrier((terms, logits, teacher))
    student_logp, teacher_logp = log_probs(logits, teacher)
    gap = jnp.exp(teacher_logp) * (teacher_logp - student_logp)
    kl_part = jnp.sum(jnp.where(mine, gap, 0.0), axis=1)
    column = local_column + (slab * 2 + half) * vt + offset(row_g)
    hit = (column == ids[:, None]) & mine
    picked = jnp.sum(jnp.where(hit, logits, 0.0), axis=1)
    loss_part = jnp.broadcast_to(jnp.sum(mask_float * kl_part), kl_part.shape)
    sent = by_group(jnp.stack([kl_part, picked, loss_part]))
    sent = jnp.broadcast_to(sent[:, None], (n_g, 2 * n_s) + sent.shape[1:])
    every = from_every(sent.reshape(-1, 3, tokens), ("g", "s", "h"))

    def for_slab(s):
        index = (half ^ (s // n_g)) * n_g + (row_g ^ (s % n_g))
        return lax.dynamic_slice_in_dim(partial, index * rows, rows, 1)

    result = for_slab(slab)
    slab_terms = [for_slab(slab ^ ms).astype(jnp.bfloat16) for ms in range(1, n_s)]
    arrived = [exchanged(term, s=ms) for ms, term in enumerate(slab_terms, 1)]
    every, _ = lax.optimization_barrier((every, slab_terms))
    token_kl, picked, core_loss = jnp.sum(every, axis=0)
    sampled = picked - top[:tokens] - log_total[:tokens]
    core_loss = jnp.broadcast_to(core_loss, (8, LANES))
    loss = (core_loss + exchanged(core_loss, c=1))[0, 0] / mask_total

    for part in arrived:
        result = result + part.astype(jnp.float32)
    return (result.astype(jnp.bfloat16), token_kl, sampled, loss)


def solution(mesh):
    n_dp, n_vocab = mesh.devices.shape
    n_g, n_s = n_dp // 2, n_vocab // 2
    split = Mesh(mesh.devices.reshape(n_g, 2, n_s, 2), ("g", "c", "s", "h"))
    dp, vocab = ("g", "c"), ("s", "h")
    return jax.shard_map(
        on_device,
        mesh=split,
        in_specs=(P(dp, vocab), P(vocab, dp, None), P(dp, vocab), P(dp), P(dp)),
        out_specs=(P(dp, vocab), P(dp), P(dp), P()),
        check_vma=False,
    )
```

```python
import functools
import math

import jax
import jax.numpy as jnp
from jax import lax
from jax.experimental import pallas as pl
from jax.experimental.pallas import tpu as pltpu
from jax.sharding import Mesh, PartitionSpec as P

LANES = 128


def exchanged(array, **flips):
    axes = tuple(flips)
    sizes = [lax.axis_size(axis) for axis in axes]
    pairs = []
    for source in range(math.prod(sizes)):
        rest, target, stride = source, 0, 1
        for axis, size in reversed(list(zip(axes, sizes))):
            target += (rest % size ^ flips[axis]) * stride
            rest, stride = rest // size, stride * size
        pairs.append((source, target))
    return lax.ppermute(array, axes, pairs)


def from_every(array, axes):
    return lax.all_to_all(array, axes, 0, 0, tiled=True)


VMEM = pl.BlockSpec(memory_space=pltpu.VMEM)
SMEM = pl.BlockSpec(memory_space=pltpu.SMEM)
ANYWHERE = pl.BlockSpec(memory_space=pltpu.HBM)


def forward_kernel(places, slabs, *refs):
    count = len(places)
    scalars, hidden, own_parts = refs[0], refs[1 : 1 + slabs], refs[1 + slabs]
    blocks, refs = refs[2 + slabs : 2 + slabs + count], refs[2 + slabs + count :]
    result, near, far, sent, held, pairs, logits, parts, sems, pair_sems, out_sems, last_sem = refs
    copies = [
        pltpu.make_async_copy(block, held.at[k], sems.at[k]) for k, block in enumerate(blocks)
    ]
    for k in range(count):
        for ms in range(slabs):

            @pl.when(scalars[2 + 3 * k] == ms)
            def _(k=k, ms=ms):
                pltpu.make_async_copy(hidden[ms], pairs.at[k], pair_sems.at[k]).start()

        copies[k].start()
    rows, width = held.shape[1:]
    chunk = count // 4
    for begin in range(0, count, chunk):
        lhs = []
        for k in range(begin, begin + chunk):
            pltpu.make_async_copy(hidden[0], pairs.at[k], pair_sems.at[k]).wait()
            even = scalars[3 + 3 * k] == 0
            lhs.append(jnp.where(even, pairs[k, :, :rows], pairs[k, :, rows:]))
            copies[k].wait()
            for side, weight in enumerate((near, far)):

                @pl.when(scalars[4 + 3 * k] == side)
                def _(k=k, weight=weight):
                    place = places[k]
                    pltpu.make_async_copy(held.at[k], weight.at[place], out_sems.at[k]).start()

        rhs = held[begin : begin + chunk].reshape(chunk * rows, width)
        term = jnp.dot(jnp.concatenate(lhs, axis=1), rhs, preferred_element_type=jnp.float32)
        logits[...] = logits[...] + term if begin else term
    leaving = pltpu.make_async_copy(logits, result, last_sem)
    leaving.start()
    values = logits[...]
    mine = lax.broadcasted_iota(jnp.int32, values.shape, 1) >= scalars[0]
    top = jnp.max(jnp.where(mine, values, -3e38), axis=1, keepdims=True)
    total = jnp.sum(jnp.where(mine, jnp.exp(values - top), 0.0), axis=1, keepdims=True)
    lane = lax.broadcasted_iota(jnp.int32, (values.shape[0], LANES), 1)
    packed = jnp.where(lane == 0, top, jnp.where(lane == 1, total, 0.0))
    parts[...] = packed.T[:8]
    tokens = own_parts.shape[1]
    groups = values.shape[0] // tokens
    for g in range(groups):
        begin = pl.multiple_of((scalars[1] ^ g) * tokens, tokens)
        both = parts[0:2, pl.ds(begin, tokens)]
        sent[:, 2 * g : 2 * g + 2, :] = jnp.broadcast_to(both, (sent.shape[0], 2, tokens))
    own = own_parts[...]
    sent[:, 2 * groups :, :] = jnp.broadcast_to(own, (sent.shape[0],) + own.shape)
    leaving.wait()
    for k in range(count):
        pltpu.make_async_copy(held.at[k], near.at[0], out_sems.at[k]).wait()


def forward(scalars, hidden, blocks, places, own_parts, receivers):
    height = hidden[0].shape[0]
    rows, width = blocks[0].shape
    count, slabs = len(blocks), len(hidden)
    extra, tokens = own_parts.shape
    kind = blocks[0].dtype
    return pl.pallas_call(
        functools.partial(forward_kernel, places, slabs),
        out_shape=[
            jax.ShapeDtypeStruct((height, width), jnp.float32),
            jax.ShapeDtypeStruct((count // 2, rows, width), kind),
            jax.ShapeDtypeStruct((count // 2, rows, width), kind),
            jax.ShapeDtypeStruct((receivers, 2 * height // tokens + extra, tokens), jnp.float32),
        ],
        in_specs=[SMEM] + [ANYWHERE] * slabs + [VMEM] + [ANYWHERE] * count,
        out_specs=[ANYWHERE, ANYWHERE, ANYWHERE, VMEM],
        scratch_shapes=[
            pltpu.VMEM((count, rows, width), kind),
            pltpu.VMEM((count,) + hidden[0].shape, kind),
            pltpu.VMEM((height, width), jnp.float32),
            pltpu.VMEM((8, height), jnp.float32),
            pltpu.SemaphoreType.DMA((count,)),
            pltpu.SemaphoreType.DMA((count,)),
            pltpu.SemaphoreType.DMA((count,)),
            pltpu.SemaphoreType.DMA,
        ],
        compiler_params=pltpu.CompilerParams(vmem_limit_bytes=62_300_000),
        cost_estimate=pl.CostEstimate(
            flops=2 * count * height * rows * width,
            bytes_accessed=4 * count * rows * width,
            transcendentals=0,
        ),
    )(scalars, *hidden, own_parts, *blocks)


def on_device(student_hidden, student_blocks, teacher_logits, token_ids, loss_mask):
    row_g, core, slab, half = (lax.axis_index(axis) for axis in ("g", "c", "s", "h"))
    n_g, n_s = lax.axis_size("g"), lax.axis_size("s")
    tokens, _ = student_hidden.shape
    piece = student_blocks[0]
    rows = piece.shape[0]
    vt = piece.shape[1] // 2
    tiles = vt // LANES
    wide_tiles = -(-tiles // n_g)
    width = wide_tiles * LANES

    def offset(g):
        return (g * (tiles - wide_tiles)) // max(n_g - 1, 1) * LANES

    plane = [(mg, mh) for mh in range(2) for mg in range(n_g)]
    others = sorted(plane[1:], key=lambda m: (m[0].bit_count() + m[1], m))

    hidden_plane = {(0, 0): student_hidden}
    for mg, mh in others:
        hidden_plane[mg, mh] = exchanged(student_hidden, g=mg, h=mh)

    def columns_of(g, h):
        return lax.dynamic_slice_in_dim(piece, h * vt + offset(g), width, 1)

    blocks = {}
    for mg, mh in others:
        cut = columns_of(row_g ^ mg, half ^ mh)
        piece, _ = lax.optimization_barrier((piece, cut))
        blocks[mg, mh, 0] = exchanged(cut, g=mg, h=mh)
    blocks[0, 0, 0] = columns_of(row_g, half)
    for mg, mh in [(0, 0)] + others:
        blocks[mg, mh, 1] = exchanged(blocks[mg, mh, 0], c=1)

    local = teacher_logits.astype(jnp.float32)
    local_max = jnp.max(local, axis=1)
    local_sum = jnp.sum(jnp.exp(local - local_max[:, None]), axis=1)
    own_mask = loss_mask.astype(jnp.float32)
    own_count = jnp.full((8, LANES), jnp.sum(own_mask))
    chip_count = own_count + exchanged(own_count, c=1)
    own_parts = jnp.stack(
        [local_max, local_sum, own_mask + 2.0 * chip_count[0, 0], token_ids.astype(jnp.float32)]
    )

    def teacher_of(g):
        return lax.dynamic_slice_in_dim(teacher_logits, offset(g), width, 1)

    teacher = [teacher_of(row_g)] + [
        exchanged(teacher_of(row_g ^ mg), g=mg) for mg in range(1, n_g)
    ]

    sides = [jnp.concatenate([hidden_plane[mg, mh] for mg in range(n_g)]) for mh in range(2)]
    plane_hidden = jnp.where(
        half == 0, jnp.concatenate(sides, axis=1), jnp.concatenate(sides[::-1], axis=1)
    )
    gathered = [plane_hidden]
    gathered += [exchanged(plane_hidden, s=ms) for ms in range(1, n_s)]

    local_column = lax.broadcasted_iota(jnp.int32, (1, width), 1)
    shared = jnp.where(row_g > 0, offset(row_g - 1) + width - offset(row_g), 0)
    mine = local_column >= shared

    crossed = core ^ half
    members = [(0, 0)] + others
    keys = [(*member, mc) for member in members[:2] for mc in range(2)]
    keys += [(*member, mc) for mc in range(2) for member in members[2:]]

    values = [shared, row_g]
    for mg, mh, mc in keys:
        values += [slab ^ ((half ^ mh) * n_g + (row_g ^ mg)), core ^ mc, crossed ^ mc]
    places = [plane.index((mg, mh)) for mg, mh, _ in keys]
    scalars = jnp.stack(values).astype(jnp.int32)
    chosen = [blocks[key] for key in keys]
    logits, *weights, sent = forward(scalars, gathered, chosen, places, own_parts, 2 * n_s * n_g)

    def by_group(stack):
        parts = stack.reshape(stack.shape[0], n_g, tokens)
        return jnp.stack(
            [lax.dynamic_index_in_dim(parts, row_g ^ g, 1, False) for g in range(n_g)]
        )

    every = from_every(sent, ("g", "s", "h"))
    teacher, _ = lax.optimization_barrier((teacher, every))
    student_parts = every[:, : 2 * n_g].reshape(2 * n_s * n_g, n_g, 2, tokens)
    student_parts = jnp.concatenate(
        [lax.dynamic_index_in_dim(student_parts, row_g ^ mg, 1, False) for mg in range(n_g)], 2
    )
    teacher_parts = every[:, 2 * n_g :].reshape(n_g, 2 * n_s, 4, tokens)
    teacher_parts = jnp.concatenate(
        [lax.dynamic_index_in_dim(teacher_parts, row_g ^ mg, 0, False) for mg in range(n_g)], 2
    )

    def normalizer(maxes, sums):
        top = jnp.max(maxes, axis=0)
        return top, jnp.log(jnp.sum(sums * jnp.exp(maxes - top), axis=0))

    top, log_total = normalizer(student_parts[:, 0], student_parts[:, 1])
    t_top, t_log = normalizer(teacher_parts[:, 0], teacher_parts[:, 1])
    coded, ids = teacher_parts[0, 2], teacher_parts[0, 3].astype(jnp.int32)
    chip_counts = jnp.floor(coded * 0.5)
    mask_float = coded - 2.0 * chip_counts
    totals = jnp.sum(chip_counts.reshape(n_g, tokens), axis=0)
    mask_total = totals[0]
    factor = (mask_float / jnp.concatenate([totals] * n_g))[:, None]

    def log_probs(logits, teacher):
        student_logp = logits - top[:, None] - log_total[:, None]
        return student_logp, teacher - t_top[:, None] - t_log[:, None]

    student_logp, teacher_logp = log_probs(logits, jnp.concatenate(teacher).astype(jnp.float32))
    delta = factor * (jnp.exp(student_logp) - jnp.exp(teacher_logp))
    dlogits = jnp.where(mine, delta, 0.0).astype(jnp.bfloat16)

    wide = len(plane) * rows

    def features_of(mh):
        return lax.dot_general(
            dlogits,
            weights[mh].reshape(wide, width),
            (((1,), (1,)), ((), ())),
            preferred_element_type=jnp.float32,
        )

    far = features_of(1)
    grads = (features_of(0), far)

    def for_half(mg, mh):
        return grads[mh][mg * tokens : (mg + 1) * tokens]

    partial = for_half(0, 0)
    terms = [for_half(mg, mh).astype(jnp.bfloat16) for mg, mh in others]
    arrived = [(exchanged(term, g=mg, h=mh), mg, mh) for term, (mg, mh) in zip(terms, others)]
    _, logits, teacher = lax.optimization_barrier((terms, logits, teacher))
    teacher = jnp.concatenate(teacher).astype(jnp.float32)
    student_logp, teacher_logp = log_probs(logits, teacher)
    gap = jnp.exp(teacher_logp) * (teacher_logp - student_logp)
    kl_part = jnp.sum(jnp.where(mine, gap, 0.0), axis=1)
    column = local_column + (slab * 2 + half) * vt + offset(row_g)
    hit = (column == ids[:, None]) & mine
    picked = jnp.sum(jnp.where(hit, logits, 0.0), axis=1)
    loss_part = jnp.broadcast_to(jnp.sum(mask_float * kl_part), kl_part.shape)
    sent = by_group(jnp.stack([kl_part, picked, loss_part]))
    sent = jnp.broadcast_to(sent[:, None], (n_g, 2 * n_s) + sent.shape[1:])
    every = from_every(sent.reshape(-1, 3, tokens), ("g", "s", "h"))

    def for_slab(s):
        total = 0.0
        for part, kg, kh in [(partial, 0, 0)] + arrived:
            index = (half ^ kh ^ (s // n_g)) * n_g + (row_g ^ kg ^ (s % n_g))
            block = lax.dynamic_slice_in_dim(part, index * rows, rows, 1)
            total = total + block.astype(jnp.float32)
        return total

    result = for_slab(slab)
    slab_terms = [for_slab(slab ^ ms).astype(jnp.bfloat16) for ms in range(1, n_s)]
    slab_parts = [exchanged(term, s=ms) for ms, term in enumerate(slab_terms, 1)]
    every, _ = lax.optimization_barrier((every, slab_terms))
    token_kl, picked, core_loss = jnp.sum(every, axis=0)
    sampled = picked - top[:tokens] - log_total[:tokens]
    core_loss = jnp.broadcast_to(core_loss, (8, LANES))
    loss = (core_loss + exchanged(core_loss, c=1))[0, 0] / mask_total

    for part in slab_parts:
        result = result + part.astype(jnp.float32)
    return (result.astype(jnp.bfloat16), token_kl, sampled, loss)


def solution(mesh):
    n_dp, n_vocab = mesh.devices.shape
    n_g, n_s = n_dp // 2, n_vocab // 2
    split = Mesh(mesh.devices.reshape(n_g, 2, n_s, 2), ("g", "c", "s", "h"))
    dp, vocab = ("g", "c"), ("s", "h")
    return jax.shard_map(
        on_device,
        mesh=split,
        in_specs=(P(dp, vocab), P(vocab, dp, None), P(dp, vocab), P(dp), P(dp)),
        out_specs=(P(dp, vocab), P(dp), P(dp), P()),
        check_vma=False,
    )
```

```python
import functools
import math

import jax
import jax.numpy as jnp
from jax import lax
from jax.experimental import pallas as pl
from jax.experimental.pallas import tpu as pltpu
from jax.sharding import Mesh, PartitionSpec as P

LANES = 128


def exchanged(array, **flips):
    axes = tuple(flips)
    sizes = [lax.axis_size(axis) for axis in axes]
    pairs = []
    for source in range(math.prod(sizes)):
        rest, target, stride = source, 0, 1
        for axis, size in reversed(list(zip(axes, sizes))):
            target += (rest % size ^ flips[axis]) * stride
            rest, stride = rest // size, stride * size
        pairs.append((source, target))
    return lax.ppermute(array, axes, pairs)


def from_every(array, axes):
    return lax.all_to_all(array, axes, 0, 0, tiled=True)


VMEM = pl.BlockSpec(memory_space=pltpu.VMEM)
SMEM = pl.BlockSpec(memory_space=pltpu.SMEM)
ANYWHERE = pl.BlockSpec(memory_space=pltpu.HBM)


def placed(scalars, k, source, near, far, place, sem):
    for side, weight in enumerate((near, far)):

        @pl.when(scalars[4 + 3 * k] == side)
        def _(weight=weight):
            pltpu.make_async_copy(source, weight.at[place], sem).start()


def stage_kernel(places, scalars, *refs):
    count = len(places)
    blocks, (near, far, held, sems, out_sems) = refs[:count], refs[count:]
    copies = [
        pltpu.make_async_copy(block, held.at[k], sems.at[k]) for k, block in enumerate(blocks)
    ]
    for copy in copies:
        copy.start()
    for k, copy in enumerate(copies):
        copy.wait()
        placed(scalars, k, held.at[k], near, far, places[k], out_sems.at[k])
    for k in range(count):
        pltpu.make_async_copy(held.at[k], near.at[0], out_sems.at[k]).wait()


def staged(scalars, blocks, places, total):
    rows, width = blocks[0].shape
    kind, count = blocks[0].dtype, len(blocks)
    return pl.pallas_call(
        functools.partial(stage_kernel, places),
        out_shape=[jax.ShapeDtypeStruct((total // 2, rows, width), kind)] * 2,
        in_specs=[SMEM] + [ANYWHERE] * count,
        out_specs=[ANYWHERE] * 2,
        scratch_shapes=[
            pltpu.VMEM((count, rows, width), kind),
            pltpu.SemaphoreType.DMA((count,)),
            pltpu.SemaphoreType.DMA((count,)),
        ],
        compiler_params=pltpu.CompilerParams(vmem_limit_bytes=64_600_000),
        cost_estimate=pl.CostEstimate(
            flops=2 * count * rows * width,
            bytes_accessed=4 * count * rows * width,
            transcendentals=0,
        ),
    )(scalars, *blocks)


def forward_kernel(places, slabs, bound, early, *refs):
    count = len(places)
    scalars, hidden, own_parts = refs[0], refs[1 : 1 + slabs], refs[1 + slabs]
    blocks, refs = refs[2 + slabs : 2 + slabs + count], refs[4 + slabs + count :]
    result, near, far, sent, held, pairs, logits, parts, sems, pair_sems, out_sems, last_sem = refs
    copies = [
        pltpu.make_async_copy(block, held.at[k], sems.at[k]) for k, block in enumerate(blocks)
    ]
    for k in range(count):
        for ms in range(slabs):

            @pl.when(scalars[2 + 3 * k] == ms)
            def _(k=k, ms=ms):
                pltpu.make_async_copy(hidden[ms], pairs.at[k], pair_sems.at[k]).start()

        copies[k].start()
    rows, width = held.shape[1:]
    chunk = count // 4
    for begin in range(0, count, chunk):
        lhs = []
        for k in range(begin, begin + chunk):
            pltpu.make_async_copy(hidden[0], pairs.at[k], pair_sems.at[k]).wait()
            even = scalars[3 + 3 * k] == 0
            lhs.append(jnp.where(even, pairs[k, :, :rows], pairs[k, :, rows:]))
            copies[k].wait()
        rhs = held[begin : begin + chunk].reshape(chunk * rows, width)
        term = jnp.dot(jnp.concatenate(lhs, axis=1), rhs, preferred_element_type=jnp.float32)
        logits[...] = logits[...] + term if begin else term
    for k in range(early, count):
        placed(scalars, k, held.at[k], near, far, places[k], out_sems.at[k])
    leaving = pltpu.make_async_copy(logits, result, last_sem)
    leaving.start()
    values, edge = logits[:, bound:], logits[:, :bound]
    mine = lax.broadcasted_iota(jnp.int32, edge.shape, 1) >= scalars[0]
    edge_top = jnp.max(jnp.where(mine, edge, -3e38), axis=1, keepdims=True)
    top = jnp.maximum(jnp.max(values, axis=1, keepdims=True), edge_top)
    total = jnp.sum(jnp.exp(values - top), axis=1, keepdims=True)
    total += jnp.sum(jnp.where(mine, jnp.exp(edge - top), 0.0), axis=1, keepdims=True)
    lane = lax.broadcasted_iota(jnp.int32, (values.shape[0], LANES), 1)
    packed = jnp.where(lane == 0, top, jnp.where(lane == 1, total, 0.0))
    parts[...] = packed.T[:8]
    tokens = own_parts.shape[1]
    groups = values.shape[0] // tokens
    for g in range(groups):
        begin = pl.multiple_of((scalars[1] ^ g) * tokens, tokens)
        both = parts[0:2, pl.ds(begin, tokens)]
        sent[:, 2 * g : 2 * g + 2, :] = jnp.broadcast_to(both, (sent.shape[0], 2, tokens))
    own = own_parts[...]
    sent[:, 2 * groups :, :] = jnp.broadcast_to(own, (sent.shape[0],) + own.shape)
    leaving.wait()
    for k in range(early, count):
        pltpu.make_async_copy(held.at[k], near.at[0], out_sems.at[k]).wait()


def forward(scalars, hidden, blocks, places, bound, early, weights, own_parts, receivers):
    height = hidden[0].shape[0]
    rows, width = blocks[0].shape
    count, slabs = len(blocks), len(hidden)
    extra, tokens = own_parts.shape
    kind = blocks[0].dtype
    return pl.pallas_call(
        functools.partial(forward_kernel, places, slabs, bound, early),
        out_shape=[
            jax.ShapeDtypeStruct((height, width), jnp.float32),
            jax.ShapeDtypeStruct((count // 2, rows, width), kind),
            jax.ShapeDtypeStruct((count // 2, rows, width), kind),
            jax.ShapeDtypeStruct((receivers, 2 * height // tokens + extra, tokens), jnp.float32),
        ],
        in_specs=[SMEM] + [ANYWHERE] * slabs + [VMEM] + [ANYWHERE] * (count + 2),
        out_specs=[ANYWHERE, ANYWHERE, ANYWHERE, VMEM],
        scratch_shapes=[
            pltpu.VMEM((count, rows, width), kind),
            pltpu.VMEM((count,) + hidden[0].shape, kind),
            pltpu.VMEM((height, width), jnp.float32),
            pltpu.VMEM((8, height), jnp.float32),
            pltpu.SemaphoreType.DMA((count,)),
            pltpu.SemaphoreType.DMA((count,)),
            pltpu.SemaphoreType.DMA((count,)),
            pltpu.SemaphoreType.DMA,
        ],
        input_output_aliases={2 + slabs + count: 1, 3 + slabs + count: 2},
        compiler_params=pltpu.CompilerParams(vmem_limit_bytes=64_600_000),
        cost_estimate=pl.CostEstimate(
            flops=2 * count * height * rows * width,
            bytes_accessed=4 * count * rows * width,
            transcendentals=0,
        ),
    )(scalars, *hidden, own_parts, *blocks, *weights)


def on_device(student_hidden, student_blocks, teacher_logits, token_ids, loss_mask):
    row_g, core, slab, half = (lax.axis_index(axis) for axis in ("g", "c", "s", "h"))
    n_g, n_s = lax.axis_size("g"), lax.axis_size("s")
    n_blocks = 4 * n_g
    tokens, _ = student_hidden.shape
    piece = student_blocks[0]
    rows = piece.shape[0]
    vt = piece.shape[1] // 2
    tiles = vt // LANES
    wide_tiles = -(-tiles // n_g)
    width = wide_tiles * LANES

    def offset(g):
        return (g * (tiles - wide_tiles)) // max(n_g - 1, 1) * LANES

    plane = [(mg, mh) for mh in range(2) for mg in range(n_g)]
    others = others_of(n_g)

    hidden_plane = {(0, 0): student_hidden}
    for mg, mh in others:
        hidden_plane[mg, mh] = exchanged(student_hidden, g=mg, h=mh)

    def columns_of(g, h):
        return lax.dynamic_slice_in_dim(piece, h * vt + offset(g), width, 1)

    blocks = {}
    for k, (mg, mh) in enumerate(others):
        cut = columns_of(row_g ^ mg, half ^ mh)
        if k:
            piece, _ = lax.optimization_barrier((piece, cut))
        blocks[mg, mh, 0] = exchanged(cut, g=mg, h=mh)
    blocks[0, 0, 0] = columns_of(row_g, half)
    for mg, mh in [(0, 0)] + others:
        blocks[mg, mh, 1] = exchanged(blocks[mg, mh, 0], c=1)

    local = teacher_logits.astype(jnp.float32)
    local_max = jnp.max(local, axis=1)
    local_sum = jnp.sum(jnp.exp(local - local_max[:, None]), axis=1)
    own_mask = loss_mask.astype(jnp.float32)
    own_count = jnp.full((8, LANES), jnp.sum(own_mask))
    chip_count = own_count + exchanged(own_count, c=1)
    own_parts = jnp.stack(
        [local_max, local_sum, own_mask + 2.0 * chip_count[0, 0], token_ids.astype(jnp.float32)]
    )

    def teacher_of(g):
        return lax.dynamic_slice_in_dim(teacher_logits, offset(g), width, 1)

    teacher = [teacher_of(row_g)] + [
        exchanged(teacher_of(row_g ^ mg), g=mg) for mg in range(1, n_g)
    ]

    student_hidden, _ = lax.optimization_barrier((student_hidden, hidden_plane[others[-1]]))
    hidden_plane[0, 0] = student_hidden
    sides = [jnp.concatenate([hidden_plane[mg, mh] for mg in range(n_g)]) for mh in range(2)]
    plane_hidden = jnp.where(
        half == 0, jnp.concatenate(sides, axis=1), jnp.concatenate(sides[::-1], axis=1)
    )
    gathered = [plane_hidden]
    gathered += [exchanged(plane_hidden, s=ms) for ms in range(1, n_s)]

    local_column = lax.broadcasted_iota(jnp.int32, (1, width), 1)
    shared = jnp.where(row_g > 0, offset(row_g - 1) + width - offset(row_g), 0)
    mine = local_column >= shared

    crossed = core ^ half
    members = [(0, 0)] + others
    keys = [(*member, mc) for member in members[:2] for mc in range(2)]
    keys += [(*member, mc) for mc in range(2) for member in members[2:]]

    values = [shared, row_g]
    for mg, mh, mc in keys:
        values += [slab ^ ((half ^ mh) * n_g + (row_g ^ mg)), core ^ mc, crossed ^ mc]
    places = [plane.index((mg, mh)) for mg, mh, _ in keys]
    bound = max([offset(g - 1) + width - offset(g) for g in range(1, n_g)] + [LANES])
    scalars = jnp.stack(values).astype(jnp.int32)
    chosen = [blocks[key] for key in keys]
    weights = staged(scalars, chosen[:4], places[:4], n_blocks)
    logits, *weights, sent = forward(
        scalars, gathered, chosen, places, bound, 4, weights, own_parts, 2 * n_s * n_g
    )

    def by_group(stack):
        parts = stack.reshape(stack.shape[0], n_g, tokens)
        return jnp.stack(
            [lax.dynamic_index_in_dim(parts, row_g ^ g, 1, False) for g in range(n_g)]
        )

    every = from_every(sent, ("g", "s", "h"))
    teacher, _ = lax.optimization_barrier((teacher, every))
    student_parts = every[:, : 2 * n_g].reshape(2 * n_s * n_g, n_g, 2, tokens)
    student_parts = jnp.concatenate(
        [lax.dynamic_index_in_dim(student_parts, row_g ^ mg, 1, False) for mg in range(n_g)], 2
    )
    teacher_parts = every[:, 2 * n_g :].reshape(n_g, 2 * n_s, 4, tokens)
    teacher_parts = jnp.concatenate(
        [lax.dynamic_index_in_dim(teacher_parts, row_g ^ mg, 0, False) for mg in range(n_g)], 2
    )

    def normalizer(maxes, sums):
        top = jnp.max(maxes, axis=0)
        return top, jnp.log(jnp.sum(sums * jnp.exp(maxes - top), axis=0))

    top, log_total = normalizer(student_parts[:, 0], student_parts[:, 1])
    t_top, t_log = normalizer(teacher_parts[:, 0], teacher_parts[:, 1])
    coded, ids = teacher_parts[0, 2], teacher_parts[0, 3].astype(jnp.int32)
    chip_counts = jnp.floor(coded * 0.5)
    mask_float = coded - 2.0 * chip_counts
    totals = jnp.sum(chip_counts.reshape(n_g, tokens), axis=0)
    mask_total = totals[0]
    factor = (mask_float / jnp.concatenate([totals] * n_g))[:, None]

    def log_probs(logits, teacher):
        student_logp = logits - top[:, None] - log_total[:, None]
        return student_logp, teacher - t_top[:, None] - t_log[:, None]

    student_logp, teacher_logp = log_probs(logits, jnp.concatenate(teacher).astype(jnp.float32))
    delta = factor * (jnp.exp(student_logp) - jnp.exp(teacher_logp))
    dlogits = jnp.where(mine, delta, 0.0).astype(jnp.bfloat16)

    wide = len(plane) * rows

    def features_of(mh):
        return lax.dot_general(
            dlogits,
            weights[mh].reshape(wide, width),
            (((1,), (1,)), ((), ())),
            preferred_element_type=jnp.float32,
        )

    grads = (features_of(0), features_of(1))

    def for_half(mg, mh):
        return grads[mh][mg * tokens : (mg + 1) * tokens]

    partial = for_half(0, 0)
    terms = [for_half(mg, mh).astype(jnp.bfloat16) for mg, mh in others]
    arrived = [(exchanged(term, g=mg, h=mh), mg, mh) for term, (mg, mh) in zip(terms, others)]
    _, logits, teacher = lax.optimization_barrier((terms, logits, teacher))
    teacher = jnp.concatenate(teacher).astype(jnp.float32)
    student_logp, teacher_logp = log_probs(logits, teacher)
    gap = jnp.exp(teacher_logp) * (teacher_logp - student_logp)
    kl_part = jnp.sum(jnp.where(mine, gap, 0.0), axis=1)
    column = local_column + (slab * 2 + half) * vt + offset(row_g)
    hit = (column == ids[:, None]) & mine
    picked = jnp.sum(jnp.where(hit, logits, 0.0), axis=1)
    loss_part = jnp.broadcast_to(jnp.sum(mask_float * kl_part), kl_part.shape)
    sent = by_group(jnp.stack([kl_part, picked, loss_part]))
    sent = jnp.broadcast_to(sent[:, None], (n_g, 2 * n_s) + sent.shape[1:])
    every = from_every(sent.reshape(-1, 3, tokens), ("g", "s", "h"))

    def for_slab(s):
        total = 0.0
        for part, kg, kh in [(partial, 0, 0)] + arrived:
            index = (half ^ kh ^ (s // n_g)) * n_g + (row_g ^ kg ^ (s % n_g))
            block = lax.dynamic_slice_in_dim(part, index * rows, rows, 1)
            total = total + block.astype(jnp.float32)
        return total

    slab_terms = [for_slab(slab ^ ms).astype(jnp.bfloat16) for ms in range(1, n_s)]
    result = for_slab(slab)
    slab_parts = [exchanged(term, s=ms) for ms, term in enumerate(slab_terms, 1)]
    every, _ = lax.optimization_barrier((every, slab_terms))
    token_kl, picked, core_loss = jnp.sum(every, axis=0)
    sampled = picked - top[:tokens] - log_total[:tokens]
    core_loss = jnp.broadcast_to(core_loss, (8, LANES))
    loss = (core_loss + exchanged(core_loss, c=1))[0, 0] / mask_total

    for part in slab_parts:
        result = result + part.astype(jnp.float32)
    return (result.astype(jnp.bfloat16), token_kl, sampled, loss)


def others_of(n_g):
    masks = [(mg, mh) for mh in range(2) for mg in range(n_g)][1:]
    return sorted(masks, key=lambda m: (m[0].bit_count() + m[1], m))


def solution(mesh):
    n_dp, n_vocab = mesh.devices.shape
    n_g, n_s = n_dp // 2, n_vocab // 2
    split = Mesh(mesh.devices.reshape(n_g, 2, n_s, 2), ("g", "c", "s", "h"))
    dp, vocab = ("g", "c"), ("s", "h")
    return jax.shard_map(
        on_device,
        mesh=split,
        in_specs=(P(dp, vocab), P(vocab, dp, None), P(dp, vocab), P(dp), P(dp)),
        out_specs=(P(dp, vocab), P(dp), P(dp), P()),
        check_vma=False,
    )
```
